32 devices in a mesh: ep: 8 (over y, x, core), tp: 4 (over z).
Axes of the slice: x: 2, y: 2, z: 4, core: 2. Of those that a mesh axis runs over, the one named last changes fastest.
Arguments:
- tokens: bfloat16 [1024, 2048], P('ep', 'tp'), may hold values from -6 to 6
- routing: int32 [1024, 8], P('ep'), may hold values from 0 to 31, all different within a row; in each aligned block of 128 rows (0 to 127, 128 to 255, ...) at most 64 rows name the same one
- gate_fixed: int32 [1024, 8], P('ep'), may hold values from 1 to 65535
- gate_weight: bfloat16 [32, 2048, 768], P('ep', 'tp'), may hold values from -0.125 to 0.125
- up_weight: bfloat16 [32, 2048, 768], P('ep', 'tp'), may hold values from -0.1875 to 0.1875
- down_weight: bfloat16 [32, 2048, 768], P('ep', 'tp'), may hold values from -0.21875 to 0.21875
Outputs:
- layer_out: bfloat16 [1024, 2048], P('ep', 'tp')
The draws below stay inside these ranges and needn't reach their ends.
Inputs may be any that keep to these rules, and one draw needn't show every extreme that they name: `routing`: each token names 8 different experts. In each aligned block of 128 tokens (the tokens of one index of ep) no expert is named by more than 64 tokens, and in some blocks one expert is named by exactly 64.
All inputs are finite; a program needn't handle non-finite values.
Results may differ from the reference program's by a relative error of at most 0.0057.
Values may be sent and summed in bfloat16 or wider, within the bound.
A program may use at most 64 MiB of HBM per device.

```python
import math
import jax
import jax.numpy as jnp
import numpy as np
from jax import lax

D = 2048
FF = 768
TOP = 8
TOK_EP = 128
EXPERTS = 32
CAP = 64
TOKENS = 1024
N_EP = 8


def set_ends(result, stream_key, smallest, high):
    extent = result.shape
    place = [jax.random.randint(jax.random.fold_in(stream_key, axis), (), 0, extent[axis]) for axis in range(len(extent))]
    result = result.at[tuple(place)].set(smallest)
    longest = extent.index(max(extent))
    place[longest] = (place[longest] + 1) % extent[longest]
    return result.at[tuple(place)].set(high)


def raised(drawn, stream_key, source, target, shards_of, factor):
    def block_of(dim):
        return (jnp.arange(drawn.shape[dim]) // (drawn.shape[dim] // shards_of)).reshape((-1,) + (1,) * (drawn.ndim - 1 - dim))

    near = jax.random.permutation(stream_key, shards_of)[block_of(target)]
    other_side = (block_of(target) + shards_of // 2) % shards_of
    return jnp.where((block_of(source) == near) | (block_of(source) == other_side), factor * drawn, drawn)


def shard_levels(stream_key, dims, cuts, least, top_value):
    loudness = 1.0
    for axis_at, shards_of in cuts:
        heights = jax.random.uniform(jax.random.fold_in(jax.random.fold_in(stream_key, 6), axis_at), (shards_of,), jnp.float32, least / len(cuts), top_value / len(cuts))
        loudness = loudness * jnp.repeat(jnp.exp(heights), dims[axis_at] // shards_of).reshape((-1,) + (1,) * (len(dims) - 1 - axis_at))
    return loudness


def shared_out(stream_key, own, number, rows, number_of, top, most, lean):
    ranking = jax.random.permutation(stream_key, number_of)
    packed, usual = load_shares(number_of, rows * top, most, lean, True), load_shares(number_of, rows * top, most, lean, False)
    places = jnp.arange(number_of)

    def named(tallies, rotation):
        used = int((tallies > 0).sum())
        fixed = max(1, used // 4)
        passed = fixed + (places - fixed + rotation * (used - fixed)) % max(1, number_of - fixed)
        return jnp.zeros((number_of,), jnp.int32).at[ranking[jnp.where(places < fixed, places, passed)]].set(jnp.asarray(tallies, jnp.int32))

    tallies = jnp.where(number % 4 == 0, named(packed, number // 4), named(usual, number - number // 4 - 1))
    mixed = jax.random.permutation(jax.random.fold_in(own, 3), number_of)
    source_of, taker = mixed[0:number_of // 2 * 2:2], mixed[1:number_of // 2 * 2:2]
    slack = jnp.minimum(tallies[source_of] - 1, most - tallies[taker]) // 2
    slack = jnp.where((source_of == ranking[0]) | (taker == ranking[0]) | (tallies[taker] == 0), 0, jnp.maximum(slack, 0))
    passed = jax.random.randint(jax.random.fold_in(own, 4), (number_of // 2,), 0, 1 << 20) % (slack + 1)
    tallies = tallies.at[source_of].add(-passed).at[taker].add(passed)
    members = jnp.searchsorted(jnp.cumsum(tallies), jnp.arange(rows * top), side="right").astype(jnp.int32)
    listing = members.reshape(top, rows).T
    listing = listing[jax.random.permutation(jax.random.fold_in(own, 1), rows)]
    rotation = jax.random.randint(jax.random.fold_in(own, 2), (rows, 1), 0, top)
    return jnp.take_along_axis(listing, (jnp.arange(top)[None, :] + rotation) % top, axis=1)


def load_shares(amount, total, most, skew, full):
    loads = [(1 << 20) // math.isqrt(standing ** skew) + 1 for standing in range(1, amount + 1)]
    largest = most if full else min(most, max(-(-total // amount), total * loads[0] // sum(loads)))
    least = 1 if total - largest >= amount - 1 else 0
    holding, spare = [largest] + [least] * (amount - 1), total - largest - least * (amount - 1)
    while spare > 0:
        free = [i for i in range(1, amount) if holding[i] < largest] or [i for i in range(1, amount) if holding[i] < most]
        mass, budget = sum([loads[i] for i in free]), spare
        for i in free:
            addition = min(most - holding[i], max(1, budget * loads[i] // mass), spare)
            holding[i] = holding[i] + addition
            spare = spare - addition
    return np.array(holding)


def centred(stream_key, shape, deviation, bound, shards=(), kind=jnp.bfloat16):
    level = shard_levels(stream_key, shape, shards, -0.22, 0.18) if shards else 1.0
    entries = jax.random.normal(stream_key, shape, jnp.float32) * deviation * level
    return jnp.minimum(jnp.maximum(entries, -bound), bound).astype(kind)


def gaussian_with(rng, shape, spread, limit, shards, heavy, kind=jnp.bfloat16):
    entries = spread * jax.random.normal(rng, shape, jnp.float32)
    if shards:
        entries = entries * shard_levels(rng, shape, shards, -0.22, 0.18)
    return jnp.clip(raised(entries, jax.random.fold_in(rng, 3), *heavy), -limit, limit).astype(kind)


def setup_inputs(seed: int = 0) -> dict:
    streams_of = jax.random.split(jax.random.key(seed), 7)
    tokens = centred(streams_of[0], (TOKENS, D), 1.0, 6.0, ((0, 8), (1, 4)))
    routing_keys = jax.random.split(jax.random.fold_in(streams_of[1], 1), TOKENS // TOK_EP)
    routing_turns = jax.random.permutation(jax.random.fold_in(streams_of[1], 3), TOKENS // TOK_EP)
    routing = jax.vmap(lambda own, number: shared_out(jax.random.fold_in(streams_of[1], 2), own, number, TOK_EP, EXPERTS, TOP, CAP, 1))(routing_keys, routing_turns).reshape((TOKENS, TOP))
    gate_fixed = set_ends(jax.random.randint(streams_of[2], (TOKENS, TOP), 1, 65536), jax.random.fold_in(streams_of[2], 1), 1, 65535).astype(jnp.int32)
    gate_weight = centred(streams_of[3], (EXPERTS, D, FF), D ** -0.5, 0.125, ((0, 8), (1, 4)))
    up_weight = gaussian_with(streams_of[4], (EXPERTS, D, FF), D ** -0.5, 0.1875, ((0, 8), (1, 4)), (1, 2, 4, 2.0))
    down_weight = centred(streams_of[5], (EXPERTS, D, FF), FF ** -0.5, 0.21875, ((0, 8), (1, 4)))
    return dict(tokens=tokens, routing=routing, gate_fixed=gate_fixed, gate_weight=gate_weight, up_weight=up_weight, down_weight=down_weight)


def slot_positions(block_ids, experts):
    one_hot = (block_ids[..., None] == jnp.arange(experts, dtype=jnp.int32)).astype(jnp.int32)
    earlier = jnp.cumsum(one_hot, axis=1) - one_hot
    return jnp.sum(earlier * one_hot, axis=-1).astype(jnp.int32)


def expert_step(operands):
    slot_rows, gate_mat, up_mat, down_mat = operands
    gate_acts = jnp.dot(slot_rows, gate_mat, preferred_element_type=jnp.float32)
    up_acts = jnp.dot(slot_rows, up_mat, preferred_element_type=jnp.float32)
    hidden = (jax.nn.silu(gate_acts) * up_acts).astype(jnp.bfloat16)
    return jnp.dot(hidden, down_mat.T, preferred_element_type=jnp.float32).astype(jnp.bfloat16)


def reference(tokens, routing, gate_fixed, gate_weight, up_weight, down_weight):
    block_ids = routing.reshape(N_EP, TOK_EP * TOP).astype(jnp.int32)
    position = slot_positions(block_ids, EXPERTS)
    block_iota = jnp.broadcast_to(jnp.arange(N_EP, dtype=jnp.int32)[:, None], block_ids.shape)
    copies = jnp.repeat(tokens, TOP, axis=0).reshape(N_EP, TOK_EP * TOP, D)
    slot_rows = jnp.zeros((EXPERTS, N_EP, CAP, D), jnp.bfloat16)
    slot_rows = slot_rows.at[block_ids, block_iota, position].set(copies)
    results = lax.map(expert_step, (slot_rows.reshape(EXPERTS, N_EP * CAP, D), gate_weight, up_weight, down_weight))
    picked = results.reshape(EXPERTS, N_EP, CAP, D)[block_ids, block_iota, position]
    scales = (gate_fixed.astype(jnp.float32) / 65536.0).reshape(N_EP, TOK_EP * TOP, 1)
    mixed = (picked.astype(jnp.float32) * scales).reshape(TOKENS, TOP, D)
    return jnp.sum(mixed, axis=1).astype(jnp.bfloat16)
```

```python
import functools

import jax
import jax.numpy as jnp
from jax import lax
from jax.experimental import pallas as pl
from jax.experimental.pallas import tpu as pltpu
from jax.sharding import PartitionSpec as P

MESH = pl.DeviceIdType.MESH
SKEW = 2


def layer_kernel(
    nep, n, local, cap, top,
    tok_ref, meta_ref, gw_hbm, uw_hbm, dw_hbm,
    out_ref,
    gw, uw, dw, tok_all, meta_all,
    ra, rb, ha, hb, pg, pu, acc, out_send, out_recv,
    w_sem, tok_s, tok_r, meta_s, meta_r,
    ra_s, ra_r, rb_s, rb_r, ha_s, ha_r, hb_s, hb_r, out_s, out_r,
):
    me = lax.axis_index("ep")
    z = lax.axis_index("tp")
    half = local // 2
    chunks = nep * half
    rows = tok_ref.shape[0]
    width = gw.shape[2]
    zl = lax.rem(z + n - 1, n)
    zr = lax.rem(z + 1, n)

    weight_copies = [
        pltpu.make_async_copy(src, dst, w_sem.at[i])
        for i, (src, dst) in enumerate(((gw_hbm, gw), (uw_hbm, uw), (dw_hbm, dw)))
    ]
    for copy in weight_copies:
        copy.start()

    barrier = pltpu.get_barrier_semaphore()

    def greet(j, carry):
        pl.semaphore_signal(
            barrier, inc=1, device_id={"ep": lax.rem(me + j, nep)}, device_id_type=MESH
        )
        return carry

    lax.fori_loop(1, nep, greet, 0)

    for side in (zl, zr):
        pl.semaphore_signal(barrier, inc=1, device_id={"tp": side}, device_id_type=MESH)
    pl.semaphore_wait(barrier, nep + 1)

    def remote(src, dst, s, r, device):
        return pltpu.make_async_remote_copy(
            src_ref=src, dst_ref=dst, send_sem=s, recv_sem=r,
            device_id=device, device_id_type=MESH,
        )

    def tok_copy(j):
        to = {"ep": lax.rem(me - j + nep, nep)}
        return remote(tok_ref, tok_all.at[j], tok_s.at[j], tok_r.at[j], to)

    def meta_copy(j):
        to = {"ep": lax.rem(me - j + nep, nep)}
        return remote(meta_ref, meta_all.at[j], meta_s.at[j], meta_r.at[j], to)

    def out_copy(j):
        to = {"ep": lax.rem(me + j, nep)}
        return remote(out_send.at[j], out_recv.at[j], out_s.at[j], out_r.at[j], to)

    def ra_copy(k):
        return remote(ra.at[k], ra.at[k], ra_s.at[k], ra_r.at[k], {"tp": zl})

    def rb_copy(k):
        return remote(rb.at[k], rb.at[k], rb_s.at[k], rb_r.at[k], {"tp": zr})

    def ha_copy(k):
        return remote(ha.at[k], ha.at[k], ha_s.at[k], ha_r.at[k], {"tp": zr})

    def hb_copy(k):
        return remote(hb.at[k], hb.at[k], hb_s.at[k], hb_r.at[k], {"tp": zl})

    def send_tokens(j, carry):
        meta_copy(j).start()
        tok_copy(j).start()
        return carry

    lax.fori_loop(1, nep, send_tokens, 0)
    tok_all[0] = tok_ref[...]
    meta_all[0] = meta_ref[...]

    def clear(j, carry):
        acc[j] = jnp.zeros(acc.shape[1:], acc.dtype)
        return carry

    lax.fori_loop(0, nep, clear, 0)
    for copy in weight_copies:
        copy.wait()

    before = (
        lax.broadcasted_iota(jnp.int32, (rows, rows), 0)
        < lax.broadcasted_iota(jnp.int32, (rows, rows), 1)
    ).astype(jnp.bfloat16)
    slot_id = lax.broadcasted_iota(jnp.int32, (cap, rows), 0).astype(jnp.float32)

    def selection(j, e):
        named = meta_all[j, :top, :] == me * local + e
        chosen = jnp.sum(named.astype(jnp.float32), axis=0, keepdims=True)
        wide = jnp.broadcast_to(chosen, (16, rows)).astype(jnp.bfloat16)
        position = jnp.dot(wide, before, preferred_element_type=jnp.float32)[:1]
        hit = jnp.where(chosen > 0.5, position, -1.0)
        return named, slot_id == hit

    def gates(j, named, picked):
        values = meta_all[j, top:, :].astype(jnp.float32) / 65536.0
        row = jnp.sum(jnp.where(named, values, 0.0), axis=0, keepdims=True)
        return jnp.sum(jnp.where(picked, row, 0.0), axis=1, keepdims=True)

    def inside(k):
        return jnp.logical_and(k >= 0, k < chunks)

    def partial_stage(k, first_expert, buf, copy, has_source, is_last, hidden):
        @pl.when(inside(k))
        def _():
            j = k // half
            e = first_expert + k % half
            _, picked = selection(j, e)
            x = jnp.dot(
                picked.astype(jnp.bfloat16), tok_all[j], preferred_element_type=jnp.float32
            ).astype(jnp.bfloat16)
            pg[...] = jnp.dot(x, gw[e], preferred_element_type=jnp.float32)
            pu[...] = jnp.dot(x, uw[e], preferred_element_type=jnp.float32)

            @pl.when(has_source)
            def _():
                copy(k).wait_recv()
                pg[...] += buf[k, :, :width].astype(jnp.float32)
                pu[...] += buf[k, :, width:].astype(jnp.float32)

            @pl.when(jnp.logical_not(is_last))
            def _():
                buf[k, :, :width] = pg[...].astype(jnp.bfloat16)
                buf[k, :, width:] = pu[...].astype(jnp.bfloat16)
                copy(k).start()

            @pl.when(is_last)
            def _():
                v = pg[...]
                hidden[k] = (v / (1.0 + jnp.exp(-v)) * pu[...]).astype(jnp.bfloat16)

    def hidden_stage(k, first_expert, hidden, copy, has_source, is_last):
        @pl.when(inside(k))
        def _():
            @pl.when(has_source)
            def _():
                copy(k).wait_recv()

            @pl.when(jnp.logical_not(is_last))
            def _():
                copy(k).start()

            j = k // half
            e = first_expert + k % half
            named, picked = selection(j, e)
            result = lax.dot_general(
                hidden[k], dw[e], (((1,), (1,)), ((), ())), preferred_element_type=jnp.float32
            )
            scaled = (result * gates(j, named, picked)).astype(jnp.bfloat16)
            acc[j] += lax.dot_general(
                picked.astype(jnp.bfloat16), scaled, (((0,), (0,)), ((), ())),
                preferred_element_type=jnp.float32,
            )

    turn = SKEW * (n - 1)
    from_right = SKEW * (n - 1 - z)
    from_left = SKEW * z

    def step(t, carry):
        k_first = t - jnp.minimum(from_left, from_right)

        @pl.when(jnp.logical_and(inside(k_first), k_first % half == 0))
        def _():
            j = k_first // half

            @pl.when(j > 0)
            def _():
                meta_copy(j).wait_recv()
                tok_copy(j).wait_recv()

        partial_stage(t - from_right, 0, ra, ra_copy, z < n - 1, z == 0, ha)
        partial_stage(t - from_left, half, rb, rb_copy, z > 0, z == n - 1, hb)
        hidden_stage(t - turn - from_left, 0, ha, ha_copy, z > 0, z == n - 1)
        hidden_stage(t - turn - from_right, half, hb, hb_copy, z < n - 1, z == 0)
        k_done = t - turn - jnp.maximum(from_left, from_right)

        @pl.when(jnp.logical_and(inside(k_done), k_done % half == half - 1))
        def _():
            j = k_done // half

            @pl.when(j > 0)
            def _():
                out_send[j] = acc[j].astype(jnp.bfloat16)
                out_copy(j).start()

        return carry

    lax.fori_loop(0, chunks + 2 * turn, step, 0)

    def finish_chunk(k, carry):
        @pl.when(z > 0)
        def _():
            ra_copy(k).wait_send()
            hb_copy(k).wait_send()

        @pl.when(z < n - 1)
        def _():
            rb_copy(k).wait_send()
            ha_copy(k).wait_send()

        return carry

    lax.fori_loop(0, chunks, finish_chunk, 0)

    def finish_block(j, carry):
        tok_copy(j).wait_send()
        meta_copy(j).wait_send()
        out_copy(j).wait_recv()
        acc[0] += out_recv[j].astype(jnp.float32)
        out_copy(j).wait_send()
        return carry

    lax.fori_loop(1, nep, finish_block, 0)
    out_ref[...] = acc[0].astype(jnp.bfloat16)


def on_device(nep, n, tokens, routing, gate_fixed, gate_weight, up_weight, down_weight):
    local, share, width = gate_weight.shape
    rows, top = routing.shape
    cap = max(2, rows * top * 2 // (local * nep))
    chunks = nep * (local // 2)
    meta = jnp.concatenate([routing.T, gate_fixed.T], axis=0)
    bf16, f32 = jnp.bfloat16, jnp.float32
    dma = pltpu.SemaphoreType.DMA
    vmem = pl.BlockSpec(memory_space=pltpu.VMEM)
    hbm = pl.BlockSpec(memory_space=pl.ANY)
    return pl.pallas_call(
        functools.partial(layer_kernel, nep, n, local, cap, top),
        out_shape=jax.ShapeDtypeStruct((rows, share), bf16),
        in_specs=[vmem, vmem, hbm, hbm, hbm],
        out_specs=vmem,
        scratch_shapes=[
            pltpu.VMEM((local, share, width), bf16),
            pltpu.VMEM((local, share, width), bf16),
            pltpu.VMEM((local, share, width), bf16),
            pltpu.VMEM((nep, rows, share), bf16),
            pltpu.VMEM((nep, 2 * top, rows), jnp.int32),
            pltpu.VMEM((chunks, cap, 2 * width), bf16),
            pltpu.VMEM((chunks, cap, 2 * width), bf16),
            pltpu.VMEM((chunks, cap, width), bf16),
            pltpu.VMEM((chunks, cap, width), bf16),
            pltpu.VMEM((cap, width), f32),
            pltpu.VMEM((cap, width), f32),
            pltpu.VMEM((nep, rows, share), f32),
            pltpu.VMEM((nep, rows, share), bf16),
            pltpu.VMEM((nep, rows, share), bf16),
            dma((3,)),
            dma((nep,)), dma((nep,)), dma((nep,)), dma((nep,)),
            dma((chunks,)), dma((chunks,)), dma((chunks,)), dma((chunks,)),
            dma((chunks,)), dma((chunks,)), dma((chunks,)), dma((chunks,)),
            dma((nep,)), dma((nep,)),
        ],
        compiler_params=pltpu.CompilerParams(
            collective_id=0, has_side_effects=True, vmem_limit_bytes=60 * 1024 * 1024
        ),
    )(tokens, meta, gate_weight, up_weight, down_weight)


def solution(mesh):
    in_specs = (
        P("ep", "tp"),
        P("ep", None),
        P("ep", None),
        P("ep", "tp", None),
        P("ep", "tp", None),
        P("ep", "tp", None),
    )
    body = functools.partial(on_device, mesh.shape["ep"], mesh.shape["tp"])
    return jax.shard_map(
        body, mesh=mesh, in_specs=in_specs, out_specs=P("ep", "tp"), check_vma=False
    )
```

```python
import functools

import jax
import jax.numpy as jnp
from jax import lax
from jax.experimental import pallas as pl
from jax.experimental.pallas import tpu as pltpu
from jax.sharding import PartitionSpec as P

MESH = pl.DeviceIdType.MESH
SKEW = 2


def layer_kernel(
    nep, n, local, cap, top,
    tok_ref, meta_ref, gw_hbm, uw_hbm, dw_hbm,
    out_ref,
    gw, uw, dw, tok_all, meta_all,
    ra, rb, ha, hb, pg, pu, acc, out_send, out_recv,
    w_sem, tok_s, tok_r, meta_s, meta_r,
    ra_s, ra_r, rb_s, rb_r, ha_s, ha_r, hb_s, hb_r, out_s, out_r,
):
    me = lax.axis_index("ep")
    z = lax.axis_index("tp")
    half = local // 2
    chunks = nep * half
    rows = tok_ref.shape[0]
    width = gw.shape[2]
    zl = lax.rem(z + n - 1, n)
    zr = lax.rem(z + 1, n)

    def weight_copy(i, e):
        src, dst = ((gw_hbm, gw), (uw_hbm, uw), (dw_hbm, dw))[i]
        return pltpu.make_async_copy(src.at[e], dst.at[e], w_sem.at[i, e])

    for i in ((0, 1), (2,)):
        for e in range(half):
            for first in (0, half):
                for which in i:
                    weight_copy(which, first + e).start()

    barrier = pltpu.get_barrier_semaphore()

    def greet(j, carry):
        pl.semaphore_signal(
            barrier, inc=1, device_id={"ep": lax.rem(me + j, nep)}, device_id_type=MESH
        )
        return carry

    lax.fori_loop(1, nep, greet, 0)

    for side in (zl, zr):
        pl.semaphore_signal(barrier, inc=1, device_id={"tp": side}, device_id_type=MESH)
    pl.semaphore_wait(barrier, nep + 1)

    def remote(src, dst, s, r, device):
        return pltpu.make_async_remote_copy(
            src_ref=src, dst_ref=dst, send_sem=s, recv_sem=r,
            device_id=device, device_id_type=MESH,
        )

    def tok_copy(j):
        to = {"ep": lax.rem(me - j + nep, nep)}
        return remote(tok_ref, tok_all.at[j], tok_s.at[j], tok_r.at[j], to)

    def meta_copy(j):
        to = {"ep": lax.rem(me - j + nep, nep)}
        return remote(meta_ref, meta_all.at[j], meta_s.at[j], meta_r.at[j], to)

    def out_copy(j):
        to = {"ep": lax.rem(me + j, nep)}
        return remote(out_send.at[j], out_recv.at[j], out_s.at[j], out_r.at[j], to)

    def ra_copy(k):
        return remote(ra.at[k], ra.at[k], ra_s.at[k], ra_r.at[k], {"tp": zl})

    def rb_copy(k):
        return remote(rb.at[k], rb.at[k], rb_s.at[k], rb_r.at[k], {"tp": zr})

    def ha_copy(k):
        return remote(ha.at[k], ha.at[k], ha_s.at[k], ha_r.at[k], {"tp": zr})

    def hb_copy(k):
        return remote(hb.at[k], hb.at[k], hb_s.at[k], hb_r.at[k], {"tp": zl})

    def send_tokens(j, carry):
        meta_copy(j).start()
        tok_copy(j).start()
        return carry

    lax.fori_loop(1, nep, send_tokens, 0)
    tok_all[0] = tok_ref[...]
    meta_all[0] = meta_ref[...]

    def clear(j, carry):
        acc[j] = jnp.zeros(acc.shape[1:], acc.dtype)
        return carry

    lax.fori_loop(0, nep, clear, 0)
    before = (
        lax.broadcasted_iota(jnp.int32, (rows, rows), 0)
        < lax.broadcasted_iota(jnp.int32, (rows, rows), 1)
    ).astype(jnp.bfloat16)
    slot_id = lax.broadcasted_iota(jnp.int32, (cap, rows), 0).astype(jnp.float32)

    def selection(j, e):
        named = meta_all[j, :top, :] == me * local + e
        chosen = jnp.sum(named.astype(jnp.float32), axis=0, keepdims=True)
        wide = jnp.broadcast_to(chosen, (16, rows)).astype(jnp.bfloat16)
        position = jnp.dot(wide, before, preferred_element_type=jnp.float32)[:1]
        hit = jnp.where(chosen > 0.5, position, -1.0)
        return named, slot_id == hit

    def gates(j, named, picked):
        values = meta_all[j, top:, :].astype(jnp.float32) / 65536.0
        row = jnp.sum(jnp.where(named, values, 0.0), axis=0, keepdims=True)
        return jnp.sum(jnp.where(picked, row, 0.0), axis=1, keepdims=True)

    def inside(k):
        return jnp.logical_and(k >= 0, k < chunks)

    def partial_stage(k, first_expert, buf, copy, has_source, is_last, hidden):
        @pl.when(inside(k))
        def _():
            j = k // half
            e = first_expert + k % half

            @pl.when(j == 0)
            def _():
                weight_copy(0, e).wait()
                weight_copy(1, e).wait()

            _, picked = selection(j, e)
            x = jnp.dot(
                picked.astype(jnp.bfloat16), tok_all[j], preferred_element_type=jnp.float32
            ).astype(jnp.bfloat16)
            pg[...] = jnp.dot(x, gw[e], preferred_element_type=jnp.float32)
            pu[...] = jnp.dot(x, uw[e], preferred_element_type=jnp.float32)

            @pl.when(has_source)
            def _():
                copy(k).wait_recv()
                pg[...] += buf[k, :, :width].astype(jnp.float32)
                pu[...] += buf[k, :, width:].astype(jnp.float32)

            @pl.when(jnp.logical_not(is_last))
            def _():
                buf[k, :, :width] = pg[...].astype(jnp.bfloat16)
                buf[k, :, width:] = pu[...].astype(jnp.bfloat16)
                copy(k).start()

            @pl.when(is_last)
            def _():
                v = pg[...]
                hidden[k] = (v / (1.0 + jnp.exp(-v)) * pu[...]).astype(jnp.bfloat16)

    def hidden_stage(k, first_expert, hidden, copy, has_source, is_last):
        @pl.when(inside(k))
        def _():
            @pl.when(has_source)
            def _():
                copy(k).wait_recv()

            @pl.when(jnp.logical_not(is_last))
            def _():
                copy(k).start()

            j = k // half
            e = first_expert + k % half

            @pl.when(j == 0)
            def _():
                weight_copy(2, e).wait()

            named, picked = selection(j, e)
            result = lax.dot_general(
                hidden[k], dw[e], (((1,), (1,)), ((), ())), preferred_element_type=jnp.float32
            )
            scaled = result * gates(j, named, picked)
            high = scaled.astype(jnp.bfloat16)
            low = (scaled - high.astype(jnp.float32)).astype(jnp.bfloat16)
            spread = picked.astype(jnp.bfloat16)
            acc[j] += lax.dot_general(
                jnp.concatenate([spread, spread], axis=0),
                jnp.concatenate([high, low], axis=0),
                (((0,), (0,)), ((), ())),
                preferred_element_type=jnp.float32,
            )

    turn = SKEW * (n - 1)
    from_right = SKEW * (n - 1 - z)
    from_left = SKEW * z

    def step(t, carry):
        k_first = t - jnp.minimum(from_left, from_right)

        @pl.when(jnp.logical_and(inside(k_first), k_first % half == 0))
        def _():
            j = k_first // half

            @pl.when(j > 0)
            def _():
                meta_copy(j).wait_recv()
                tok_copy(j).wait_recv()

        partial_stage(t - from_right, 0, ra, ra_copy, z < n - 1, z == 0, ha)
        partial_stage(t - from_left, half, rb, rb_copy, z > 0, z == n - 1, hb)
        hidden_stage(t - turn - from_left, 0, ha, ha_copy, z > 0, z == n - 1)
        hidden_stage(t - turn - from_right, half, hb, hb_copy, z < n - 1, z == 0)
        k_done = t - turn - jnp.maximum(from_left, from_right)

        @pl.when(jnp.logical_and(inside(k_done), k_done % half == half - 1))
        def _():
            j = k_done // half

            @pl.when(j > 0)
            def _():
                out_send[j] = acc[j].astype(jnp.bfloat16)
                out_copy(j).start()

        return carry

    lax.fori_loop(0, chunks + 2 * turn, step, 0)

    def finish_chunk(k, carry):
        @pl.when(z > 0)
        def _():
            ra_copy(k).wait_send()
            hb_copy(k).wait_send()

        @pl.when(z < n - 1)
        def _():
            rb_copy(k).wait_send()
            ha_copy(k).wait_send()

        return carry

    lax.fori_loop(0, chunks, finish_chunk, 0)

    def finish_block(j, carry):
        tok_copy(j).wait_send()
        meta_copy(j).wait_send()
        out_copy(j).wait_recv()
        acc[0] += out_recv[j].astype(jnp.float32)
        out_copy(j).wait_send()
        return carry

    lax.fori_loop(1, nep, finish_block, 0)
    out_ref[...] = acc[0].astype(jnp.bfloat16)


def on_device(nep, n, tokens, routing, gate_fixed, gate_weight, up_weight, down_weight):
    local, share, width = gate_weight.shape
    rows, top = routing.shape
    cap = max(2, rows * top * 2 // (local * nep))
    chunks = nep * (local // 2)
    meta = jnp.concatenate([routing.T, gate_fixed.T], axis=0)
    bf16, f32 = jnp.bfloat16, jnp.float32
    dma = pltpu.SemaphoreType.DMA
    vmem = pl.BlockSpec(memory_space=pltpu.VMEM)
    hbm = pl.BlockSpec(memory_space=pl.ANY)
    return pl.pallas_call(
        functools.partial(layer_kernel, nep, n, local, cap, top),
        out_shape=jax.ShapeDtypeStruct((rows, share), bf16),
        in_specs=[vmem, vmem, hbm, hbm, hbm],
        out_specs=vmem,
        scratch_shapes=[
            pltpu.VMEM((local, share, width), bf16),
            pltpu.VMEM((local, share, width), bf16),
            pltpu.VMEM((local, share, width), bf16),
            pltpu.VMEM((nep, rows, share), bf16),
            pltpu.VMEM((nep, 2 * top, rows), jnp.int32),
            pltpu.VMEM((chunks, cap, 2 * width), bf16),
            pltpu.VMEM((chunks, cap, 2 * width), bf16),
            pltpu.VMEM((chunks, cap, width), bf16),
            pltpu.VMEM((chunks, cap, width), bf16),
            pltpu.VMEM((cap, width), f32),
            pltpu.VMEM((cap, width), f32),
            pltpu.VMEM((nep, rows, share), f32),
            pltpu.VMEM((nep, rows, share), bf16),
            pltpu.VMEM((nep, rows, share), bf16),
            dma((3, local)),
            dma((nep,)), dma((nep,)), dma((nep,)), dma((nep,)),
            dma((chunks,)), dma((chunks,)), dma((chunks,)), dma((chunks,)),
            dma((chunks,)), dma((chunks,)), dma((chunks,)), dma((chunks,)),
            dma((nep,)), dma((nep,)),
        ],
        compiler_params=pltpu.CompilerParams(
            collective_id=0, has_side_effects=True, vmem_limit_bytes=60 * 1024 * 1024
        ),
    )(tokens, meta, gate_weight, up_weight, down_weight)


def solution(mesh):
    in_specs = (
        P("ep", "tp"),
        P("ep", None),
        P("ep", None),
        P("ep", "tp", None),
        P("ep", "tp", None),
        P("ep", "tp", None),
    )
    body = functools.partial(on_device, mesh.shape["ep"], mesh.shape["tp"])
    return jax.shard_map(
        body, mesh=mesh, in_specs=in_specs, out_specs=P("ep", "tp"), check_vma=False
    )
```
